32 devices in a mesh: dp: 16 (over z, y, core), tensor: 2 (over x).
Axes of the slice: x: 2, y: 2, z: 4, core: 2. Of those that a mesh axis runs over, the one named last changes fastest.
Arguments:
- activations: bfloat16 [32768, 1024], P(('dp', 'tensor')), may hold values from -6 to 6
- gradients: bfloat16 [32768, 5472], P('dp', 'tensor'), may hold values from -6 to 6
- act_history: float32 [2, 16, 1024], P('tensor'), may hold values from 0.1 to 4
- grad_history: float32 [16, 5472], P(None, 'tensor'), may hold values from 0.1 to 4
- owner_rank: int32 [1024], replicated, may hold values from 0 to 1
- history_slot: int32 [6496], replicated, may hold values from 0 to 15
Outputs:
- weight_grad: float32 [1024, 5472], P('dp', 'tensor')
- act_history_out: float32 [2, 16, 1024], P('tensor')
- grad_history_out: float32 [16, 5472], P(None, 'tensor')
The draws below stay inside these ranges and needn't reach their ends.
All inputs are finite; a program needn't handle non-finite values.
Results may differ from the reference program's by a relative error of at most 0.0042.
Values may be sent and summed in bfloat16 or wider, within the bound.
A program may use at most 64 MiB of HBM per device.

```python
import math
import jax
import jax.numpy as jnp
from jax import lax

D = 1024
FF = 5472
HIST = 16
TOKENS = 32768
N_TENSOR = 2


def set_ends(values, own_key, least, high):
    longest = values.shape.index(max(values.shape))
    spots = []
    for shift in (0, 1):
        where = [jax.random.randint(jax.random.fold_in(own_key, axis), (), 0, length) for axis, length in enumerate(values.shape)]
        where[longest] = (where[longest] + shift) % values.shape[longest]
        spots.append(tuple(where))
    return values.at[spots[0]].set(least).at[spots[1]].set(high)


def with_spikes(values, own_key, source, target, shards_of, factor):
    owner, partner = [(jnp.arange(values.shape[dim]) // (values.shape[dim] // shards_of)).reshape([-1 if axis == dim else 1 for axis in range(values.ndim)]) for dim in (source, target)]
    chosen = jax.random.permutation(own_key, shards_of)[partner]
    strong = (owner == chosen) | (owner == (partner + shards_of // 2) % shards_of)
    return jnp.where(strong, factor * values, values)


def shard_levels(stream_key, shape, cuts, least, largest):
    def one(position, shards_of):
        draws = jax.random.uniform(jax.random.fold_in(jax.random.fold_in(stream_key, 6), position), (shards_of,), jnp.float32, least / len(cuts), largest / len(cuts))
        return jnp.repeat(jnp.exp(draws), shape[position] // shards_of).reshape((-1,) + (1,) * (len(shape) - position - 1))

    factor_of = one(*cuts[0])
    for cut in cuts[1:]:
        factor_of = factor_of * one(*cut)
    return factor_of


def gaussian(key, shape, width, limit, split=(), held_as=jnp.bfloat16):
    result = jax.random.normal(key, shape, jnp.float32) * width
    if len(split) > 0:
        result = shard_levels(key, shape, split, -0.22, 0.18) * result
    return jnp.clip(result, min=-limit, max=limit).astype(held_as)


def bell_draw_with(own_key, shape, deviation, most, split, heavy, held_as=jnp.bfloat16):
    result = deviation * jax.random.normal(own_key, shape, jnp.float32)
    if split:
        result = result * shard_levels(own_key, shape, split, -0.22, 0.18)
    return jnp.clip(with_spikes(result, jax.random.fold_in(own_key, 3), *heavy), -most, most).astype(held_as)


def setup_inputs(seed: int = 0) -> dict:
    splits = jax.random.split(jax.random.key(seed), 7)
    return {
        "activations": bell_draw_with(splits[0], (TOKENS, D), 1.0, 6.0, ((0, 32),), (0, 1, 32, 2.75)),
        "gradients": gaussian(splits[1], (TOKENS, FF), 1.0, 6.0, ((0, 16), (1, 2))),
        "act_history": jnp.clip(jnp.exp(math.log(4.0) - 3.6888794 * jax.random.uniform(splits[2], (N_TENSOR, HIST, D), jnp.float32) ** shard_levels(splits[2], (N_TENSOR, HIST, D), ((0, 2),), -0.2, 0.2)), 0.1, 4.0),
        "grad_history": jnp.clip(jnp.exp(math.log(4.0) - 3.6888794 * jax.random.uniform(splits[3], (HIST, FF), jnp.float32) ** shard_levels(splits[3], (HIST, FF), ((1, 2),), -0.2, 0.2)), 0.1, 4.0),
        "owner_rank": set_ends(jax.random.randint(splits[4], (D,), 0, N_TENSOR), jax.random.fold_in(splits[4], 1), 0, N_TENSOR - 1).astype(jnp.int32),
        "history_slot": set_ends(jax.random.randint(splits[5], (D + FF,), 0, HIST), jax.random.fold_in(splits[5], 1), 0, HIST - 1).astype(jnp.int32),
    }


QUANT_LIMIT = 448.0
SCALE_FLOOR = 0.25

def quantize(values, scale):
    scaled = values.astype(jnp.float32) * scale
    return jnp.clip(scaled, -QUANT_LIMIT, QUANT_LIMIT).astype(jnp.bfloat16)

def place_peaks(history, peaks, slots):
    rows = lax.broadcasted_iota(jnp.int32, history.shape, 0)
    return jnp.where(rows == slots.astype(jnp.int32)[None, :], peaks[None, :], history)

def reference(activations, gradients, act_history, grad_history, owner_rank, history_slot):
    ranks = lax.broadcasted_iota(jnp.int32, act_history.shape, 0)
    picked = jnp.where(ranks == owner_rank.astype(jnp.int32)[None, None, :], act_history, jnp.float32(0.0))
    current_history = lax.optimization_barrier(jnp.sum(picked, axis=0))
    act_scale = QUANT_LIMIT / jnp.maximum(lax.optimization_barrier(jnp.max(current_history, axis=0)), SCALE_FLOOR)
    grad_scale = QUANT_LIMIT / jnp.maximum(lax.optimization_barrier(jnp.max(grad_history, axis=0)), SCALE_FLOOR)
    act_quant = quantize(activations, act_scale)
    block_width = FF // 4
    results = []
    for block_index in range(4):
        first_col = block_index * block_width
        grad_block = quantize(gradients[:, first_col:first_col + block_width], grad_scale[first_col:first_col + block_width])
        results.append(jnp.dot(act_quant.T, grad_block, preferred_element_type=jnp.float32))
    summed = jnp.concatenate(results, axis=1)
    grad_factor = 1.0 / math.sqrt(TOKENS)
    weight_grad = summed / (act_scale[:, None] * grad_scale[None, :]) * grad_factor
    act_peak = lax.optimization_barrier(jnp.max(jnp.abs(activations), axis=0)).astype(jnp.float32)
    grad_peak = lax.optimization_barrier(jnp.max(jnp.abs(gradients), axis=0)).astype(jnp.float32)
    updated = place_peaks(current_history, act_peak, history_slot[:D])
    act_history_out = jnp.broadcast_to(updated[None], (N_TENSOR, HIST, D))
    grad_history_out = place_peaks(grad_history, grad_peak, history_slot[D:])
    return (weight_grad, act_history_out, grad_history_out)
```

```python
import functools
import math

import jax
import jax.numpy as jnp
from jax import lax
from jax.experimental import pallas as pl
from jax.experimental.pallas import tpu as pltpu
from jax.sharding import PartitionSpec as P

QUANT_LIMIT = 448.0
SCALE_FLOOR = 0.25
CORES = 2
ROWS_Y = 2
LANES = 128
COL_TILE = 512
MESH = pl.DeviceIdType.MESH


def quantize(values, scale):
    scaled = values.astype(jnp.float32) * scale
    return jnp.clip(scaled, -QUANT_LIMIT, QUANT_LIMIT).astype(jnp.bfloat16)


def place_peaks(history, peaks, slots):
    rows = lax.broadcasted_iota(jnp.int32, history.shape, 0)
    return jnp.where(rows == slots[None, :], peaks[None, :], history)


def col_tiles(width):
    return [(start, min(COL_TILE, width - start)) for start in range(0, width, COL_TILE)]


def fused_kernel(
    dp, tensor,
    act_hbm, grad_hbm, act_hist_ref, grad_hist_ref, owner_ref,
    summed_ref, cur_ref, act_peak_ref, grad_peak_ref,
    act_own, act_got, hist_got, gq, part, core_got, y_out, y_got, z_out, z_got,
    lhs, peaks, act_peaks, act_scale, grad_scale,
    load_sem, grad_sem, hist_send, hist_recv, x_send, x_recv, core_send, core_recv,
    y_send, y_recv, z_send, z_recv, pk_send, pk_recv, ap_send, ap_recv,
):
    me = lax.axis_index("dp")
    mt = lax.axis_index("tensor")
    core = lax.rem(me, CORES)
    chip = lax.div(me, CORES)
    yy = lax.rem(chip, ROWS_Y)
    zz = lax.div(chip, ROWS_Y)
    depth = dp // (CORES * ROWS_Y)
    tokens, width = act_hbm.shape
    rows, cols = grad_hbm.shape
    block = width // dp
    pair = block * CORES
    tiles = col_tiles(cols)
    load_rows = rows // grad_sem.shape[0]

    def dp_index(z, y, c):
        return (z * ROWS_Y + y) * CORES + c

    sibling = dp_index(zz, yy, 1 - core)
    y_peer = dp_index(zz, 1 - yy, core)

    def grad_load(i):
        at = pl.ds(pl.multiple_of(i * load_rows, load_rows), load_rows)
        return pltpu.make_async_copy(grad_hbm.at[at], gq.at[at], grad_sem.at[i])

    def start_load(i, carry):
        grad_load(i).start()
        return carry

    act_load = pltpu.make_async_copy(act_hbm, act_own, load_sem)
    act_load.start()
    lax.fori_loop(0, grad_sem.shape[0], start_load, 0)

    barrier = pltpu.get_barrier_semaphore()
    for t in range(1, tensor):
        pl.semaphore_signal(
            barrier, inc=1, device_id={"tensor": lax.rem(mt + t, tensor)}, device_id_type=MESH
        )

    def greet(k, carry):
        pl.semaphore_signal(
            barrier, inc=1, device_id={"dp": lax.rem(me + k, dp)}, device_id_type=MESH
        )
        return carry

    lax.fori_loop(1, dp, greet, 0)
    pl.semaphore_wait(barrier, dp - 1 + tensor - 1)

    def target_z(u):
        return lax.rem(zz + 1 + u, depth)

    def block_cols(u, k):
        y = 1 - yy if k == 0 else yy
        return pl.ds(pl.multiple_of((target_z(u) * ROWS_Y + y) * pair, LANES), pair)

    def hist_copy(t):
        return pltpu.make_async_remote_copy(
            src_ref=act_hist_ref.at[0], dst_ref=hist_got.at[t - 1],
            send_sem=hist_send.at[t - 1], recv_sem=hist_recv.at[t - 1],
            device_id={"tensor": lax.rem(mt + t, tensor)}, device_id_type=MESH,
        )

    def x_copy(t, u, k):
        at = block_cols(u, k)
        return pltpu.make_async_remote_copy(
            src_ref=act_hbm.at[:, at], dst_ref=act_got.at[t - 1, :, at],
            send_sem=x_send.at[t - 1, u * 2 + k], recv_sem=x_recv.at[t - 1, u * 2 + k],
            device_id={"tensor": lax.rem(mt + t, tensor)}, device_id_type=MESH,
        )

    def core_copy(s):
        return pltpu.make_async_remote_copy(
            src_ref=part.at[s, pl.ds(pl.multiple_of((1 - core) * block, block), block)],
            dst_ref=core_got.at[s],
            send_sem=core_send.at[s], recv_sem=core_recv.at[s],
            device_id={"dp": sibling}, device_id_type=MESH,
        )

    def y_copy(u):
        return pltpu.make_async_remote_copy(
            src_ref=y_out.at[u], dst_ref=y_got.at[u],
            send_sem=y_send.at[u], recv_sem=y_recv.at[u],
            device_id={"dp": y_peer}, device_id_type=MESH,
        )

    def z_copy(u):
        return pltpu.make_async_remote_copy(
            src_ref=z_out.at[u], dst_ref=z_got.at[u],
            send_sem=z_send.at[u], recv_sem=z_recv.at[u],
            device_id={"dp": dp_index(target_z(u), yy, core)}, device_id_type=MESH,
        )

    def peak_copy(k):
        return pltpu.make_async_remote_copy(
            src_ref=peaks.at[0], dst_ref=peaks.at[k],
            send_sem=pk_send.at[k - 1], recv_sem=pk_recv.at[k - 1],
            device_id={"dp": lax.rem(me + k, dp)}, device_id_type=MESH,
        )

    def act_peak_copy(t):
        return pltpu.make_async_remote_copy(
            src_ref=act_peaks.at[0], dst_ref=act_peaks.at[t],
            send_sem=ap_send.at[t - 1], recv_sem=ap_recv.at[t - 1],
            device_id={"tensor": lax.rem(mt + t, tensor)}, device_id_type=MESH,
        )

    for t in range(1, tensor):
        hist_copy(t).start()

    def start_x(u, carry):
        for k in range(2):
            for t in range(1, tensor):
                x_copy(t, u, k).start()
        return carry

    lax.fori_loop(0, depth, start_x, 0)

    grad_scale[...] = QUANT_LIMIT / jnp.maximum(
        jnp.max(grad_hist_ref[...], axis=0, keepdims=True), SCALE_FLOOR
    )

    act_load.wait()
    step_rows = min(64, tokens)
    for start, size in col_tiles(width):
        def peak_rows(r, top, start=start, size=size):
            at = pl.ds(pl.multiple_of(r * step_rows, step_rows), step_rows)
            mag = jnp.abs(act_own[at, start:start + size])
            return jnp.maximum(top, jnp.max(mag.reshape(step_rows // 16, 16, size), axis=0))

        top = lax.fori_loop(
            0, tokens // step_rows, peak_rows, jnp.zeros((16, size), jnp.bfloat16)
        )
        peaks[0, :, start:start + size] = jnp.max(
            top.astype(jnp.float32), axis=0, keepdims=True
        )
    peaks[0, :, width:] = jnp.zeros((1, cols), jnp.float32)

    def grad_chunk(i, carry):
        grad_load(i).wait()
        for start, size in tiles:
            scale = grad_scale[:, start:start + size]

            def quant_rows(r, top, start=start, size=size, scale=scale):
                at = pl.ds(
                    pl.multiple_of(i * load_rows + r * step_rows, step_rows), step_rows
                )
                raw = gq[at, start:start + size]
                mag = jnp.abs(raw)
                gq[at, start:start + size] = quantize(raw, scale)
                return jnp.maximum(top, jnp.max(mag.reshape(step_rows // 16, 16, size), axis=0))

            top = lax.fori_loop(
                0, load_rows // step_rows, quant_rows, jnp.zeros((16, size), jnp.bfloat16)
            )
            here = slice(width + start, width + start + size)
            peaks[0, :, here] = jnp.maximum(
                peaks[0, :, here], jnp.max(top.astype(jnp.float32), axis=0, keepdims=True)
            )
        return carry

    lax.fori_loop(0, grad_sem.shape[0], grad_chunk, 0)

    def start_peak(k, carry):
        peak_copy(k).start()
        return carry

    lax.fori_loop(1, dp, start_peak, 0)

    owner = owner_ref[...]
    current = jnp.where(owner == mt, act_hist_ref[0], 0.0)
    for t in range(1, tensor):
        hist_copy(t).wait()
        source = lax.rem(mt + tensor - t, tensor)
        current = jnp.where(owner == source, hist_got[t - 1], current)
    cur_ref[...] = current
    act_scale[...] = QUANT_LIMIT / jnp.maximum(
        jnp.max(current, axis=0, keepdims=True), SCALE_FLOOR
    )

    def load_lhs(read, at):
        scaled = read.astype(jnp.float32) * act_scale[:, at]
        scaled = jnp.clip(scaled, -QUANT_LIMIT, QUANT_LIMIT)
        lhs[...] = jnp.transpose(scaled).astype(jnp.bfloat16)

    def multiply(s, source, first):
        at = pl.ds(pl.multiple_of(source * tokens, tokens), tokens)
        full = cols // COL_TILE

        def one(start, size):
            here = pl.ds(start, size)
            term = jnp.dot(lhs[...], gq[at, here], preferred_element_type=jnp.float32)
            if first:
                part[s, :, here] = term
            else:
                part[s, :, here] += term

        def tile(j, carry):
            one(pl.multiple_of(j * COL_TILE, COL_TILE), COL_TILE)
            return carry

        lax.fori_loop(0, full, tile, 0)
        if cols % COL_TILE:
            one(full * COL_TILE, cols % COL_TILE)

    mine = pl.ds(pl.multiple_of(core * block, block), block)

    def block_step(u, k):
        s = u * 2 + k
        at = block_cols(u, k)
        load_lhs(act_own[:, at], at)
        multiply(s, mt, True)
        for t in range(1, tensor):
            x_copy(t, u, k).wait_recv()
            load_lhs(act_got[t - 1, :, at], at)
            multiply(s, lax.rem(mt + tensor - t, tensor), False)
        core_copy(s).start()
        core_copy(s).wait_recv()
        both = part[s, mine, :] + core_got[s]
        if k == 0:
            y_out[u] = both.astype(jnp.bfloat16)
            y_copy(u).start()
        else:
            part[s, mine, :] = both

    def send_z(u):
        y_copy(u).wait_recv()
        z_out[u] = (part[u * 2 + 1, mine, :] + y_got[u].astype(jnp.float32)).astype(jnp.bfloat16)
        z_copy(u).start()

    def unit(u, carry):
        block_step(u, 0)

        @pl.when(u >= 1)
        def _():
            send_z(u - 1)

        block_step(u, 1)
        return carry

    lax.fori_loop(0, depth, unit, 0)

    def wait_peak(k, carry):
        peak_copy(k).wait()
        return carry

    lax.fori_loop(1, dp, wait_peak, 0)
    tops = jnp.max(peaks[...], axis=0)
    grad_peak_ref[...] = tops[:, width:]
    act_peaks[0] = tops[:, :width]
    for t in range(1, tensor):
        act_peak_copy(t).start()

    y_copy(depth - 1).wait_recv()
    total = part[depth * 2 - 1, mine, :] + y_got[depth - 1].astype(jnp.float32)
    for u in range(depth - 1):
        z_copy(u).wait_recv()
        total = total + z_got[u].astype(jnp.float32)
    summed_ref[...] = total

    for t in range(1, tensor):
        act_peak_copy(t).wait()
    act_peak_ref[...] = jnp.max(act_peaks[...], axis=0)

    def finish(u, carry):
        for k in range(2):
            for t in range(1, tensor):
                x_copy(t, u, k).wait_send()
            core_copy(u * 2 + k).wait_send()
        y_copy(u).wait_send()
        return carry

    lax.fori_loop(0, depth, finish, 0)

    def finish_z(u, carry):
        z_copy(u).wait_send()
        return carry

    lax.fori_loop(0, depth - 1, finish_z, 0)


def fused_sums(activations, gradients, act_history, grad_history, owner_rank):
    dp, tensor = lax.axis_size("dp"), lax.axis_size("tensor")
    tokens, width = activations.shape
    rows, cols = gradients.shape
    hist = act_history.shape[1]
    depth = dp // (CORES * ROWS_Y)
    steps = depth * ROWS_Y
    block = width // dp
    loads = 8
    dma = pltpu.SemaphoreType.DMA
    vmem = pl.BlockSpec(memory_space=pltpu.VMEM)
    hbm = pl.BlockSpec(memory_space=pl.ANY)
    f32, bf16 = jnp.float32, jnp.bfloat16
    others = tensor - 1
    return pl.pallas_call(
        functools.partial(fused_kernel, dp, tensor),
        out_shape=(
            jax.ShapeDtypeStruct((block, cols), f32),
            jax.ShapeDtypeStruct((hist, width), f32),
            jax.ShapeDtypeStruct((1, width), f32),
            jax.ShapeDtypeStruct((1, cols), f32),
        ),
        in_specs=[hbm, hbm, vmem, vmem, vmem],
        out_specs=(vmem, vmem, vmem, vmem),
        scratch_shapes=[
            pltpu.VMEM((tokens, width), bf16),
            pltpu.VMEM((others, tokens, width), bf16),
            pltpu.VMEM((others, hist, width), f32),
            pltpu.VMEM((rows, cols), bf16),
            pltpu.VMEM((steps, block * CORES, cols), f32),
            pltpu.VMEM((steps, block, cols), f32),
            pltpu.VMEM((depth, block, cols), bf16),
            pltpu.VMEM((depth, block, cols), bf16),
            pltpu.VMEM((depth, block, cols), bf16),
            pltpu.VMEM((depth, block, cols), bf16),
            pltpu.VMEM((block * CORES, tokens), bf16),
            pltpu.VMEM((dp, 1, width + cols), f32),
            pltpu.VMEM((tensor, 1, width), f32),
            pltpu.VMEM((1, width), f32),
            pltpu.VMEM((1, cols), f32),
            dma, dma((loads,)), dma((others,)), dma((others,)),
            dma((others, steps)), dma((others, steps)), dma((steps,)), dma((steps,)),
            dma((depth,)), dma((depth,)), dma((depth,)), dma((depth,)),
            dma((dp - 1,)), dma((dp - 1,)), dma((others,)), dma((others,)),
        ],
        compiler_params=pltpu.CompilerParams(
            collective_id=0, has_side_effects=True, vmem_limit_bytes=60 * 1024 * 1024
        ),
    )(activations, gradients, act_history, grad_history, owner_rank[None, :])


def gathered_sums(activations, gradients, act_history, grad_history, owner_rank):
    my_rank = lax.axis_index("tensor")
    held = jnp.where(owner_rank[None, :] == my_rank, act_history[0], jnp.float32(0.0))
    current = lax.psum(held, "tensor")
    act_scale = QUANT_LIMIT / jnp.maximum(jnp.max(current, axis=0), SCALE_FLOOR)
    grad_scale = QUANT_LIMIT / jnp.maximum(jnp.max(grad_history, axis=0), SCALE_FLOOR)
    gathered_rows = lax.all_gather(quantize(activations, act_scale), "tensor", axis=0, tiled=True)
    summed = lax.psum_scatter(
        lax.dot_general(
            gathered_rows, quantize(gradients, grad_scale), (((0,), (0,)), ((), ())),
            preferred_element_type=jnp.float32,
        ),
        "dp", scatter_dimension=0, tiled=True,
    )
    act_peak = lax.pmax(jnp.max(jnp.abs(activations), axis=0).astype(jnp.float32), ("dp", "tensor"))
    grad_peak = lax.pmax(jnp.max(jnp.abs(gradients), axis=0).astype(jnp.float32), "dp")
    return summed, current, act_peak[None, :], grad_peak[None, :]


def body(activations, gradients, act_history, grad_history, owner_rank, history_slot):
    dp = lax.axis_size("dp")
    model_width = act_history.shape[2]
    column_total = gradients.shape[1]
    row_count = model_width // dp
    fits = dp % (CORES * ROWS_Y) == 0 and (row_count * CORES) % LANES == 0
    sums = fused_sums if fits else gathered_sums
    summed, current, act_peak, grad_peak = sums(
        activations, gradients, act_history, grad_history, owner_rank
    )
    act_scale = QUANT_LIMIT / jnp.maximum(jnp.max(current, axis=0), SCALE_FLOOR)
    grad_scale = QUANT_LIMIT / jnp.maximum(jnp.max(grad_history, axis=0), SCALE_FLOOR)
    grad_factor = 1.0 / math.sqrt(gradients.shape[0] * dp)
    row_base = lax.axis_index("dp") * row_count
    row_scale = lax.dynamic_slice_in_dim(act_scale, row_base, row_count, 0)
    weight_grad = summed / (row_scale[:, None] * grad_scale[None, :]) * grad_factor
    act_slots = history_slot[:model_width]
    grad_slots = lax.dynamic_slice_in_dim(
        history_slot, model_width + lax.axis_index("tensor") * column_total, column_total, 0
    )
    act_history_out = place_peaks(current, act_peak[0], act_slots)[None]
    grad_history_out = place_peaks(grad_history, grad_peak[0], grad_slots)
    return (weight_grad, act_history_out, grad_history_out)


def solution(mesh):
    placed = (
        P(("dp", "tensor"), None),
        P("dp", "tensor"),
        P("tensor", None, None),
        P(None, "tensor"),
        P(),
        P(),
    )
    return jax.shard_map(
        body,
        mesh=mesh,
        in_specs=placed,
        out_specs=(P("dp", "tensor"), P("tensor", None, None), P(None, "tensor")),
        check_vma=False,
    )
```

```python
import functools
import math

import jax
import jax.numpy as jnp
from jax import lax
from jax.experimental import pallas as pl
from jax.experimental.pallas import tpu as pltpu
from jax.sharding import PartitionSpec as P

QUANT_LIMIT = 448.0
SCALE_FLOOR = 0.25
CORES = 2
ROWS_Y = 2
LANES = 128
SUBLANES = 16
COL_TILE = 512
MESH = pl.DeviceIdType.MESH


def quantize(values, scale):
    scaled = values.astype(jnp.float32) * scale
    return jnp.clip(scaled, -QUANT_LIMIT, QUANT_LIMIT).astype(jnp.bfloat16)


def place_peaks(history, peaks, slots):
    rows = lax.broadcasted_iota(jnp.int32, history.shape, 0)
    return jnp.where(rows == slots[None, :], peaks[None, :], history)


def col_tiles(width):
    return [(start, min(COL_TILE, width - start)) for start in range(0, width, COL_TILE)]


def fused_kernel(
    dp, tensor,
    act_hbm, grad_hbm, act_hist_ref, grad_hist_ref, owner_ref, act_slot_ref, grad_slot_ref,
    weight_ref, act_hist_out, grad_hist_out,
    act_own, act_got, hist_got, gq, part, core_got, y_out, y_got, z_out, z_got,
    lhs, peaks, act_peaks, act_scale, grad_scale, scale_down, peak_down, row_undo, current_hist,
    load_sem, grad_sem, hist_send, hist_recv, x_send, x_recv, core_send, core_recv,
    y_send, y_recv, z_send, z_recv, pk_send, pk_recv, ap_send, ap_recv,
):
    me = lax.axis_index("dp")
    mt = lax.axis_index("tensor")
    core = lax.rem(me, CORES)
    chip = lax.div(me, CORES)
    yy = lax.rem(chip, ROWS_Y)
    zz = lax.div(chip, ROWS_Y)
    depth = dp // (CORES * ROWS_Y)
    tokens, width = act_hbm.shape
    cols, rows = grad_hbm.shape
    block = width // dp
    pair = block * CORES
    load_cols = cols // grad_sem.shape[0]
    padded = grad_scale.shape[1]

    def dp_index(z, y, c):
        return (z * ROWS_Y + y) * CORES + c

    sibling = dp_index(zz, yy, 1 - core)
    y_peer = dp_index(zz, 1 - yy, core)

    def grad_load(i):
        at = pl.ds(pl.multiple_of(i * load_cols, SUBLANES), load_cols)
        return pltpu.make_async_copy(grad_hbm.at[at], gq.at[at], grad_sem.at[i])

    def start_load(i, carry):
        grad_load(i).start()
        return carry

    act_load = pltpu.make_async_copy(act_hbm, act_own, load_sem)
    act_load.start()
    lax.fori_loop(0, grad_sem.shape[0], start_load, 0)

    barrier = pltpu.get_barrier_semaphore()
    for t in range(1, tensor):
        pl.semaphore_signal(
            barrier, inc=1, device_id={"tensor": lax.rem(mt + t, tensor)}, device_id_type=MESH
        )

    def greet(k, carry):
        pl.semaphore_signal(
            barrier, inc=1, device_id={"dp": lax.rem(me + k, dp)}, device_id_type=MESH
        )
        return carry

    lax.fori_loop(1, dp, greet, 0)
    pl.semaphore_wait(barrier, dp - 1 + tensor - 1)

    def target_z(u):
        return lax.rem(zz + 1 + u, depth)

    def block_cols(u, k):
        y = yy * k + (1 - yy) * (1 - k)
        return pl.ds(pl.multiple_of((target_z(u) * ROWS_Y + y) * pair, LANES), pair)

    def hist_copy(t):
        return pltpu.make_async_remote_copy(
            src_ref=act_hist_ref.at[0], dst_ref=hist_got.at[t - 1],
            send_sem=hist_send.at[t - 1], recv_sem=hist_recv.at[t - 1],
            device_id={"tensor": lax.rem(mt + t, tensor)}, device_id_type=MESH,
        )

    def x_copy(t, u, k):
        at = block_cols(u, k)
        return pltpu.make_async_remote_copy(
            src_ref=act_hbm.at[:, at], dst_ref=act_got.at[t - 1, :, at],
            send_sem=x_send.at[t - 1, u * 2 + k], recv_sem=x_recv.at[t - 1, u * 2 + k],
            device_id={"tensor": lax.rem(mt + t, tensor)}, device_id_type=MESH,
        )

    def core_copy(s):
        return pltpu.make_async_remote_copy(
            src_ref=part.at[s, pl.ds(pl.multiple_of((1 - core) * block, block), block)],
            dst_ref=core_got.at[s],
            send_sem=core_send.at[s], recv_sem=core_recv.at[s],
            device_id={"dp": sibling}, device_id_type=MESH,
        )

    def y_copy(u):
        return pltpu.make_async_remote_copy(
            src_ref=y_out.at[u], dst_ref=y_got.at[u],
            send_sem=y_send.at[u], recv_sem=y_recv.at[u],
            device_id={"dp": y_peer}, device_id_type=MESH,
        )

    def z_copy(u):
        return pltpu.make_async_remote_copy(
            src_ref=z_out.at[u], dst_ref=z_got.at[u],
            send_sem=z_send.at[u], recv_sem=z_recv.at[u],
            device_id={"dp": dp_index(target_z(u), yy, core)}, device_id_type=MESH,
        )

    def peak_copy(k):
        return pltpu.make_async_remote_copy(
            src_ref=peaks.at[0], dst_ref=peaks.at[k],
            send_sem=pk_send.at[k - 1], recv_sem=pk_recv.at[k - 1],
            device_id={"dp": lax.rem(me + k, dp)}, device_id_type=MESH,
        )

    def act_peak_copy(t):
        return pltpu.make_async_remote_copy(
            src_ref=act_peaks.at[0], dst_ref=act_peaks.at[t],
            send_sem=ap_send.at[t - 1], recv_sem=ap_recv.at[t - 1],
            device_id={"tensor": lax.rem(mt + t, tensor)}, device_id_type=MESH,
        )

    for t in range(1, tensor):
        hist_copy(t).start()

    def send_x(u, k):
        for t in range(1, tensor):
            x_copy(t, u, k).start()

    def send_pair(u, carry):
        send_x(u + 1, 0)
        send_x(u, 1)
        return carry

    send_x(0, 0)
    lax.fori_loop(0, depth - 1, send_pair, 0)
    send_x(depth - 1, 1)

    grad_scale[:, padded - LANES:] = jnp.ones((1, LANES), jnp.float32)
    grad_scale[:, :cols] = QUANT_LIMIT / jnp.maximum(
        jnp.max(grad_hist_ref[...], axis=0, keepdims=True), SCALE_FLOOR
    )
    peak_down[padded - LANES:, :] = jnp.zeros((LANES, LANES), jnp.float32)

    def turn_scale(j, carry):
        at = pl.ds(pl.multiple_of(j * LANES, LANES), LANES)
        scale_down[at, :] = jnp.transpose(jnp.broadcast_to(grad_scale[:, at], (LANES, LANES)))
        return carry

    lax.fori_loop(0, padded // LANES, turn_scale, 0)

    act_load.wait()
    step_rows = min(64, tokens)
    for start, size in col_tiles(width):
        def peak_rows(r, top, start=start, size=size):
            at = pl.ds(pl.multiple_of(r * step_rows, step_rows), step_rows)
            mag = jnp.abs(act_own[at, start:start + size])
            return jnp.maximum(top, jnp.max(mag.reshape(step_rows // 16, 16, size), axis=0))

        top = lax.fori_loop(
            0, tokens // step_rows, peak_rows, jnp.zeros((16, size), jnp.bfloat16)
        )
        peaks[0, :, start:start + size] = jnp.max(
            top.astype(jnp.float32), axis=0, keepdims=True
        )
    def grad_chunk(i, carry):
        grad_load(i).wait()

        def quant_cols(j, inner):
            at = pl.ds(pl.multiple_of(i * load_cols + j * SUBLANES, SUBLANES), SUBLANES)
            scale = scale_down[at, :]
            top = jnp.zeros((SUBLANES, LANES), jnp.bfloat16)
            for start in range(0, rows, LANES):
                raw = gq[at, start:start + LANES]
                top = jnp.maximum(top, jnp.abs(raw))
                gq[at, start:start + LANES] = quantize(raw, scale)
            peak_down[at, :] = top.astype(jnp.float32)
            return inner

        return lax.fori_loop(0, load_cols // SUBLANES, quant_cols, carry)

    lax.fori_loop(0, grad_sem.shape[0], grad_chunk, 0)

    def turn_peak(j, carry):
        at = pl.ds(pl.multiple_of(j * LANES, LANES), LANES)
        turned = jnp.transpose(peak_down[at, :])
        here = pl.ds(pl.multiple_of(width + j * LANES, LANES), LANES)
        peaks[0, :, here] = jnp.max(turned, axis=0, keepdims=True)
        return carry

    lax.fori_loop(0, padded // LANES, turn_peak, 0)

    def start_peak(k, carry):
        peak_copy(k).start()
        return carry

    lax.fori_loop(1, dp, start_peak, 0)

    owner = owner_ref[...]
    current = jnp.where(owner == mt, act_hist_ref[0], 0.0)
    for t in range(1, tensor):
        hist_copy(t).wait()
        source = lax.rem(mt + tensor - t, tensor)
        current = jnp.where(owner == source, hist_got[t - 1], current)
    current_hist[...] = current
    act_scale[...] = QUANT_LIMIT / jnp.maximum(
        jnp.max(current, axis=0, keepdims=True), SCALE_FLOOR
    )

    def load_lhs(read, at):
        scaled = read.astype(jnp.float32) * act_scale[:, at]
        scaled = jnp.clip(scaled, -QUANT_LIMIT, QUANT_LIMIT)
        lhs[...] = jnp.transpose(scaled).astype(jnp.bfloat16)

    def multiply(s, source, first):
        at = pl.ds(pl.multiple_of(source * tokens, tokens), tokens)
        full = cols // COL_TILE

        def one(start, size):
            here = pl.ds(start, size)
            term = lax.dot_general(
                lhs[...], gq[here, at], (((1,), (1,)), ((), ())),
                preferred_element_type=jnp.float32,
            )
            if first:
                part[s, :, here] = term
            else:
                part[s, :, here] += term

        def tile(j, carry):
            one(pl.multiple_of(j * COL_TILE, COL_TILE), COL_TILE)
            return carry

        lax.fori_loop(0, full, tile, 0)
        if cols % COL_TILE:
            one(full * COL_TILE, cols % COL_TILE)

    mine = pl.ds(pl.multiple_of(core * block, block), block)

    def own_product(u, k):
        at = block_cols(u, k)
        load_lhs(act_own[:, at], at)
        multiply(u * 2 + k, mt, True)

    def got_product(u, k):
        at = block_cols(u, k)
        for t in range(1, tensor):
            x_copy(t, u, k).wait_recv()
            load_lhs(act_got[t - 1, :, at], at)
            multiply(u * 2 + k, lax.rem(mt + tensor - t, tensor), False)
        core_copy(u * 2 + k).start()

    def core_sum(u, k):
        core_copy(u * 2 + k).wait_recv()
        return part[u * 2 + k, mine, :] + core_got[u * 2 + k]

    def send_y(u):
        y_out[u] = core_sum(u, 0).astype(jnp.bfloat16)
        y_copy(u).start()

    def line_sum(u):
        y_copy(u).wait_recv()
        return core_sum(u, 1) + y_got[u].astype(jnp.float32)

    own_product(0, 0)
    got_product(0, 0)
    own_product(*((1, 0) if depth > 1 else (0, 1)))
    send_y(0)

    def unit(u, carry):
        got_product(u + 1, 0)
        own_product(u, 1)
        send_y(u + 1)
        got_product(u, 1)
        last = lax.div(u + 2, depth)
        own_product(u + 2 - last, last)
        z_out[u] = line_sum(u).astype(jnp.bfloat16)
        z_copy(u).start()
        return carry

    lax.fori_loop(0, depth - 1, unit, 0)

    def wait_peak(k, carry):
        peak_copy(k).wait()
        return carry

    lax.fori_loop(1, dp, wait_peak, 0)
    tops = jnp.max(peaks[...], axis=0)
    act_peaks[0] = tops[:, :width]
    for t in range(1, tensor):
        act_peak_copy(t).start()
    hist_row = lax.broadcasted_iota(jnp.int32, grad_hist_ref.shape, 0)
    grad_hist_out[...] = jnp.where(
        hist_row == grad_slot_ref[...], tops[:, width:width + cols], grad_hist_ref[...]
    )

    picks = lax.broadcasted_iota(jnp.int32, (block, width), 1) == (
        lax.broadcasted_iota(jnp.int32, (block, width), 0) + me * block
    )
    row_scale = jnp.sum(jnp.where(picks, act_scale[...], 0.0), axis=1, keepdims=True)
    row_undo[...] = jnp.broadcast_to(1.0 / row_scale, row_undo.shape)
    factor = 1.0 / math.sqrt(rows * dp)
    grad_scale[...] = factor / grad_scale[...]

    for t in range(1, tensor):
        act_peak_copy(t).wait()
    hist_row = lax.broadcasted_iota(jnp.int32, current_hist.shape, 0)
    act_hist_out[0] = jnp.where(
        hist_row == act_slot_ref[...], jnp.max(act_peaks[...], axis=0), current_hist[...]
    )

    got_product(depth - 1, 1)
    total = line_sum(depth - 1)
    for u in range(depth - 1):
        z_copy(u).wait_recv()
        total = total + z_got[u].astype(jnp.float32)
    weight_ref[...] = total * row_undo[:, :1] * grad_scale[:, :cols]

    def finish(u, carry):
        for k in range(2):
            for t in range(1, tensor):
                x_copy(t, u, k).wait_send()
            core_copy(u * 2 + k).wait_send()
        y_copy(u).wait_send()
        return carry

    lax.fori_loop(0, depth, finish, 0)

    def finish_z(u, carry):
        z_copy(u).wait_send()
        return carry

    lax.fori_loop(0, depth - 1, finish_z, 0)


def fused_outputs(activations, gradients, act_history, grad_history, owner_rank, act_slots, grad_slots):
    dp, tensor = lax.axis_size("dp"), lax.axis_size("tensor")
    tokens, width = activations.shape
    rows, cols = gradients.shape
    hist = act_history.shape[1]
    depth = dp // (CORES * ROWS_Y)
    steps = depth * ROWS_Y
    block = width // dp
    loads = max(n for n in range(1, 13) if (cols // SUBLANES) % n == 0)
    padded = pl.cdiv(cols, LANES) * LANES
    dma = pltpu.SemaphoreType.DMA
    vmem = pl.BlockSpec(memory_space=pltpu.VMEM)
    hbm = pl.BlockSpec(memory_space=pl.ANY)
    f32, bf16 = jnp.float32, jnp.bfloat16
    others = tensor - 1
    return pl.pallas_call(
        functools.partial(fused_kernel, dp, tensor),
        out_shape=(
            jax.ShapeDtypeStruct((block, cols), f32),
            jax.ShapeDtypeStruct((1, hist, width), f32),
            jax.ShapeDtypeStruct((hist, cols), f32),
        ),
        in_specs=[hbm, hbm, vmem, vmem, vmem, vmem, vmem],
        out_specs=(vmem, vmem, vmem),
        scratch_shapes=[
            pltpu.VMEM((tokens, width), bf16),
            pltpu.VMEM((others, tokens, width), bf16),
            pltpu.VMEM((others, hist, width), f32),
            pltpu.VMEM((cols, rows), bf16),
            pltpu.VMEM((steps, block * CORES, cols), f32),
            pltpu.VMEM((steps, block, cols), f32),
            pltpu.VMEM((depth, block, cols), bf16),
            pltpu.VMEM((depth, block, cols), bf16),
            pltpu.VMEM((depth, block, cols), bf16),
            pltpu.VMEM((depth, block, cols), bf16),
            pltpu.VMEM((block * CORES, tokens), bf16),
            pltpu.VMEM((dp, 1, width + padded), f32),
            pltpu.VMEM((tensor, 1, width), f32),
            pltpu.VMEM((1, width), f32),
            pltpu.VMEM((1, padded), f32),
            pltpu.VMEM((padded, LANES), f32),
            pltpu.VMEM((padded, LANES), f32),
            pltpu.VMEM((block, LANES), f32),
            pltpu.VMEM((hist, width), f32),
            dma, dma((loads,)), dma((others,)), dma((others,)),
            dma((others, steps)), dma((others, steps)), dma((steps,)), dma((steps,)),
            dma((depth,)), dma((depth,)), dma((depth,)), dma((depth,)),
            dma((dp - 1,)), dma((dp - 1,)), dma((others,)), dma((others,)),
        ],
        compiler_params=pltpu.CompilerParams(
            collective_id=0, has_side_effects=True, vmem_limit_bytes=60 * 1024 * 1024
        ),
    )(
        activations, gradients.T, act_history, grad_history,
        owner_rank[None, :], act_slots[None, :], grad_slots[None, :],
    )


def gathered_sums(activations, gradients, act_history, grad_history, owner_rank):
    my_rank = lax.axis_index("tensor")
    held = jnp.where(owner_rank[None, :] == my_rank, act_history[0], jnp.float32(0.0))
    current = lax.psum(held, "tensor")
    act_scale = QUANT_LIMIT / jnp.maximum(jnp.max(current, axis=0), SCALE_FLOOR)
    grad_scale = QUANT_LIMIT / jnp.maximum(jnp.max(grad_history, axis=0), SCALE_FLOOR)
    gathered_rows = lax.all_gather(quantize(activations, act_scale), "tensor", axis=0, tiled=True)
    summed = lax.psum_scatter(
        lax.dot_general(
            gathered_rows, quantize(gradients, grad_scale), (((0,), (0,)), ((), ())),
            preferred_element_type=jnp.float32,
        ),
        "dp", scatter_dimension=0, tiled=True,
    )
    act_peak = lax.pmax(jnp.max(jnp.abs(activations), axis=0).astype(jnp.float32), ("dp", "tensor"))
    grad_peak = lax.pmax(jnp.max(jnp.abs(gradients), axis=0).astype(jnp.float32), "dp")
    return summed, current, act_peak[None, :], grad_peak[None, :]


def body(activations, gradients, act_history, grad_history, owner_rank, history_slot):
    dp = lax.axis_size("dp")
    model_width = act_history.shape[2]
    column_total = gradients.shape[1]
    row_count = model_width // dp
    fits = dp % (CORES * ROWS_Y) == 0 and (row_count * CORES) % LANES == 0
    fits = fits and column_total % SUBLANES == 0
    act_slots = history_slot[:model_width]
    grad_slots = lax.dynamic_slice_in_dim(
        history_slot, model_width + lax.axis_index("tensor") * column_total, column_total, 0
    )
    if fits:
        return fused_outputs(
            activations, gradients, act_history, grad_history, owner_rank, act_slots, grad_slots
        )
    summed, current, act_peak, grad_peak = gathered_sums(
        activations, gradients, act_history, grad_history, owner_rank
    )
    act_scale = QUANT_LIMIT / jnp.maximum(jnp.max(current, axis=0), SCALE_FLOOR)
    grad_scale = QUANT_LIMIT / jnp.maximum(jnp.max(grad_history, axis=0), SCALE_FLOOR)
    grad_factor = 1.0 / math.sqrt(gradients.shape[0] * dp)
    row_base = lax.axis_index("dp") * row_count
    row_scale = lax.dynamic_slice_in_dim(act_scale, row_base, row_count, 0)
    weight_grad = summed / (row_scale[:, None] * grad_scale[None, :]) * grad_factor
    act_history_out = place_peaks(current, act_peak[0], act_slots)[None]
    grad_history_out = place_peaks(grad_history, grad_peak[0], grad_slots)
    return (weight_grad, act_history_out, grad_history_out)


def solution(mesh):
    placed = (
        P(("dp", "tensor"), None),
        P("dp", "tensor"),
        P("tensor", None, None),
        P(None, "tensor"),
        P(),
        P(),
    )
    return jax.shard_map(
        body,
        mesh=mesh,
        in_specs=placed,
        out_specs=(P("dp", "tensor"), P("tensor", None, None), P(None, "tensor")),
        check_vma=False,
    )
```

```python
import functools
import math

import jax
import jax.numpy as jnp
from jax import lax
from jax.experimental import pallas as pl
from jax.experimental.pallas import tpu as pltpu
from jax.sharding import PartitionSpec as P

QUANT_LIMIT = 448.0
SCALE_FLOOR = 0.25
CORES = 2
ROWS_Y = 2
LANES = 128
SUBLANES = 16
COL_TILE = 1408
MESH = pl.DeviceIdType.MESH


def quantize(values, scale):
    scaled = values.astype(jnp.float32) * scale
    return jnp.clip(scaled, -QUANT_LIMIT, QUANT_LIMIT).astype(jnp.bfloat16)


def place_peaks(history, peaks, slots):
    rows = lax.broadcasted_iota(jnp.int32, history.shape, 0)
    return jnp.where(rows == slots[None, :], peaks[None, :], history)


def col_tiles(width):
    return [(start, min(COL_TILE, width - start)) for start in range(0, width, COL_TILE)]


def fused_kernel(
    dp, tensor,
    act_hbm, grad_hbm, act_hist_ref, grad_hist_ref, owner_ref, slot_ref,
    weight_ref, act_hist_out, grad_hist_out,
    act_own, act_got, hist_got, gq, part, core_got, y_out, y_got, z_out, z_got,
    lhs, peaks, act_peaks, act_scale, grad_scale, scale_down, peak_down, row_undo, current_hist,
    load_sem, grad_sem, hist_send, hist_recv, x_send, x_recv, core_send, core_recv,
    y_send, y_recv, z_send, z_recv, pk_send, pk_recv, ap_send, ap_recv,
):
    me = lax.axis_index("dp")
    mt = lax.axis_index("tensor")
    core = lax.rem(me, CORES)
    chip = lax.div(me, CORES)
    yy = lax.rem(chip, ROWS_Y)
    zz = lax.div(chip, ROWS_Y)
    depth = dp // (CORES * ROWS_Y)
    tokens, width = act_hbm.shape
    cols, rows = grad_hbm.shape
    block = width // dp
    pair = block * CORES
    load_cols = cols // grad_sem.shape[0]
    padded = grad_scale.shape[1]

    def dp_index(z, y, c):
        return (z * ROWS_Y + y) * CORES + c

    sibling = dp_index(zz, yy, 1 - core)
    y_peer = dp_index(zz, 1 - yy, core)

    def grad_load(i):
        at = pl.ds(pl.multiple_of(i * load_cols, SUBLANES), load_cols)
        return pltpu.make_async_copy(grad_hbm.at[at], gq.at[at], grad_sem.at[i])

    def start_load(i, carry):
        grad_load(i).start()
        return carry

    act_load = pltpu.make_async_copy(act_hbm, act_own, load_sem)
    act_load.start()
    lax.fori_loop(0, grad_sem.shape[0], start_load, 0)

    barrier = pltpu.get_barrier_semaphore()
    for t in range(1, tensor):
        pl.semaphore_signal(
            barrier, inc=1, device_id={"tensor": lax.rem(mt + t, tensor)}, device_id_type=MESH
        )

    def greet(k, carry):
        pl.semaphore_signal(
            barrier, inc=1, device_id={"dp": lax.rem(me + k, dp)}, device_id_type=MESH
        )
        return carry

    lax.fori_loop(1, dp, greet, 0)
    pl.semaphore_wait(barrier, dp - 1 + tensor - 1)

    def target_z(u):
        return lax.rem(zz + 1 + u, depth)

    def block_cols(u, k):
        y = yy * k + (1 - yy) * (1 - k)
        return pl.ds(pl.multiple_of((target_z(u) * ROWS_Y + y) * pair, LANES), pair)

    def line_cols(u):
        return pl.ds(pl.multiple_of(target_z(u) * (ROWS_Y * pair), LANES), ROWS_Y * pair)

    def hist_copy(t):
        return pltpu.make_async_remote_copy(
            src_ref=act_hist_ref.at[0], dst_ref=hist_got.at[t - 1],
            send_sem=hist_send.at[t - 1], recv_sem=hist_recv.at[t - 1],
            device_id={"tensor": lax.rem(mt + t, tensor)}, device_id_type=MESH,
        )

    def x_copy(t, u, k):
        at = block_cols(u, k)
        return pltpu.make_async_remote_copy(
            src_ref=act_hbm.at[:, at], dst_ref=act_got.at[t - 1, :, at],
            send_sem=x_send.at[t - 1, u * 2 + k], recv_sem=x_recv.at[t - 1, u * 2 + k],
            device_id={"tensor": lax.rem(mt + t, tensor)}, device_id_type=MESH,
        )

    def side(k):
        return yy * k + (1 - yy) * (1 - k)

    def half_rows(k, c):
        return pl.ds(pl.multiple_of(side(k) * pair + c * block, block), block)

    def core_copy(u, k):
        s = u * 2 + k
        return pltpu.make_async_remote_copy(
            src_ref=part.at[u, half_rows(k, 1 - core)], dst_ref=core_got.at[s],
            send_sem=core_send.at[s], recv_sem=core_recv.at[s],
            device_id={"dp": sibling}, device_id_type=MESH,
        )

    def y_copy(u):
        return pltpu.make_async_remote_copy(
            src_ref=y_out.at[u], dst_ref=y_got.at[u],
            send_sem=y_send.at[u], recv_sem=y_recv.at[u],
            device_id={"dp": y_peer}, device_id_type=MESH,
        )

    def z_copy(u):
        return pltpu.make_async_remote_copy(
            src_ref=z_out.at[u], dst_ref=z_got.at[u],
            send_sem=z_send.at[u], recv_sem=z_recv.at[u],
            device_id={"dp": dp_index(target_z(u), yy, core)}, device_id_type=MESH,
        )

    def peak_copy(k):
        return pltpu.make_async_remote_copy(
            src_ref=peaks.at[0], dst_ref=peaks.at[k],
            send_sem=pk_send.at[k - 1], recv_sem=pk_recv.at[k - 1],
            device_id={"dp": lax.rem(me + k, dp)}, device_id_type=MESH,
        )

    def act_peak_copy(t):
        return pltpu.make_async_remote_copy(
            src_ref=act_peaks.at[0], dst_ref=act_peaks.at[t],
            send_sem=ap_send.at[t - 1], recv_sem=ap_recv.at[t - 1],
            device_id={"tensor": lax.rem(mt + t, tensor)}, device_id_type=MESH,
        )

    for t in range(1, tensor):
        hist_copy(t).start()

    def send_x(u, k):
        for t in range(1, tensor):
            x_copy(t, u, k).start()

    def send_pair(u, carry):
        send_x(u + 1, 0)
        send_x(u, 1)
        return carry

    send_x(0, 0)
    lax.fori_loop(0, depth - 1, send_pair, 0)
    send_x(depth - 1, 1)

    grad_scale[:, padded - LANES:] = jnp.ones((1, LANES), jnp.float32)
    grad_scale[:, :cols] = QUANT_LIMIT / jnp.maximum(
        jnp.max(grad_hist_ref[...], axis=0, keepdims=True), SCALE_FLOOR
    )
    peak_down[padded - LANES:, :] = jnp.zeros((LANES, LANES), jnp.float32)

    def turn_scale(j, carry):
        at = pl.ds(pl.multiple_of(j * LANES, LANES), LANES)
        scale_down[at, :] = jnp.transpose(jnp.broadcast_to(grad_scale[:, at], (LANES, LANES)))
        return carry

    lax.fori_loop(0, padded // LANES, turn_scale, 0)

    act_load.wait()
    step_rows = min(64, tokens)
    for start, size in col_tiles(width):
        def peak_rows(r, top, start=start, size=size):
            at = pl.ds(pl.multiple_of(r * step_rows, step_rows), step_rows)
            mag = jnp.abs(act_own[at, start:start + size])
            return jnp.maximum(top, jnp.max(mag.reshape(step_rows // 16, 16, size), axis=0))

        top = lax.fori_loop(
            0, tokens // step_rows, peak_rows, jnp.zeros((16, size), jnp.bfloat16)
        )
        peaks[0, :, start:start + size] = jnp.max(
            top.astype(jnp.float32), axis=0, keepdims=True
        )
    def grad_chunk(i, carry):
        grad_load(i).wait()

        def quant_cols(j, inner):
            at = pl.ds(pl.multiple_of(i * load_cols + j * SUBLANES, SUBLANES), SUBLANES)
            scale = scale_down[at, :]
            top = jnp.zeros((SUBLANES, LANES), jnp.bfloat16)
            for start in range(0, rows, LANES):
                raw = gq[at, start:start + LANES]
                top = jnp.maximum(top, jnp.abs(raw))
                gq[at, start:start + LANES] = quantize(raw, scale)
            peak_down[at, :] = top.astype(jnp.float32)
            return inner

        return lax.fori_loop(0, load_cols // SUBLANES, quant_cols, carry)

    lax.fori_loop(0, grad_sem.shape[0], grad_chunk, 0)

    def turn_peak(j, carry):
        at = pl.ds(pl.multiple_of(j * LANES, LANES), LANES)
        turned = jnp.transpose(peak_down[at, :])
        here = pl.ds(pl.multiple_of(width + j * LANES, LANES), LANES)
        peaks[0, :, here] = jnp.max(turned, axis=0, keepdims=True)
        return carry

    lax.fori_loop(0, padded // LANES, turn_peak, 0)

    def start_peak(k, carry):
        peak_copy(k).start()
        return carry

    lax.fori_loop(1, dp, start_peak, 0)

    owner = owner_ref[...]
    current = jnp.where(owner == mt, act_hist_ref[0], 0.0)
    for t in range(1, tensor):
        hist_copy(t).wait()
        source = lax.rem(mt + tensor - t, tensor)
        current = jnp.where(owner == source, hist_got[t - 1], current)
    current_hist[...] = current
    act_scale[...] = QUANT_LIMIT / jnp.maximum(
        jnp.max(current, axis=0, keepdims=True), SCALE_FLOOR
    )

    def load_lhs(read, at):
        return jnp.transpose(quantize(read, act_scale[:, at]))

    def multiply(put, left, source):
        at = pl.ds(pl.multiple_of(source * tokens, tokens), tokens)
        full = cols // COL_TILE

        def one(start, size):
            here = pl.ds(start, size)
            put(here, lax.dot_general(
                left[...], gq[here, at], (((1,), (1,)), ((), ())),
                preferred_element_type=jnp.float32,
            ))

        def tile(j, carry):
            one(pl.multiple_of(j * COL_TILE, COL_TILE), COL_TILE)
            return carry

        lax.fori_loop(0, full, tile, 0)
        if cols % COL_TILE:
            one(full * COL_TILE, cols % COL_TILE)

    def own_product(u):
        at = line_cols(u)
        lhs[...] = load_lhs(act_own[:, at], at)

        def put(here, term):
            part[u, :, here] = term

        multiply(put, lhs, mt)

    def got_product(u, k):
        at = block_cols(u, k)
        down = pl.ds(pl.multiple_of(side(k) * pair, pair), pair)

        def put(here, term):
            part[u, down, here] += term

        for t in range(1, tensor):
            x_copy(t, u, k).wait_recv()
            lhs[:pair, :] = load_lhs(act_got[t - 1, :, at], at)
            multiply(put, lhs.at[:pair], lax.rem(mt + tensor - t, tensor))
        core_copy(u, k).start()

    def core_sum(u, k):
        core_copy(u, k).wait_recv()
        return part[u, half_rows(k, core), :] + core_got[u * 2 + k]

    def send_y(u):
        y_out[u] = core_sum(u, 0).astype(jnp.bfloat16)
        y_copy(u).start()

    def line_sum(u):
        y_copy(u).wait_recv()
        return core_sum(u, 1) + y_got[u].astype(jnp.float32)

    own_product(0)
    got_product(0, 0)
    if depth > 1:
        own_product(1)
    send_y(0)

    def unit(u, carry):
        got_product(u + 1, 0)

        @pl.when(u + 2 < depth)
        def _():
            own_product(u + 2)

        send_y(u + 1)
        got_product(u, 1)
        z_out[u] = line_sum(u).astype(jnp.bfloat16)
        z_copy(u).start()
        return carry

    lax.fori_loop(0, depth - 1, unit, 0)

    def wait_peak(k, carry):
        peak_copy(k).wait()
        return carry

    lax.fori_loop(1, dp, wait_peak, 0)
    tops = jnp.max(peaks[...], axis=0)
    act_peaks[0] = tops[:, :width]
    for t in range(1, tensor):
        act_peak_copy(t).start()
    hist_row = lax.broadcasted_iota(jnp.int32, grad_hist_ref.shape, 0)
    grad_slots = slot_ref[:, width:width + cols]
    for t in range(1, tensor):
        first = width + t * cols
        grad_slots = jnp.where(mt == t, slot_ref[:, first:first + cols], grad_slots)
    grad_hist_out[...] = jnp.where(
        hist_row == grad_slots, tops[:, width:width + cols], grad_hist_ref[...]
    )

    picks = lax.broadcasted_iota(jnp.int32, (block, width), 1) == (
        lax.broadcasted_iota(jnp.int32, (block, width), 0) + me * block
    )
    row_scale = jnp.sum(jnp.where(picks, act_scale[...], 0.0), axis=1, keepdims=True)
    row_undo[...] = jnp.broadcast_to(1.0 / row_scale, row_undo.shape)
    factor = 1.0 / math.sqrt(rows * dp)
    grad_scale[...] = factor / grad_scale[...]

    for t in range(1, tensor):
        act_peak_copy(t).wait()
    hist_row = lax.broadcasted_iota(jnp.int32, current_hist.shape, 0)
    act_hist_out[0] = jnp.where(
        hist_row == slot_ref[:, :width], jnp.max(act_peaks[...], axis=0), current_hist[...]
    )

    got_product(depth - 1, 1)
    total = line_sum(depth - 1)
    for u in range(depth - 1):
        z_copy(u).wait_recv()
        total = total + z_got[u].astype(jnp.float32)
    weight_ref[...] = total * row_undo[:, :1] * grad_scale[:, :cols]

    def finish(u, carry):
        for k in range(2):
            for t in range(1, tensor):
                x_copy(t, u, k).wait_send()
            core_copy(u, k).wait_send()
        y_copy(u).wait_send()
        return carry

    lax.fori_loop(0, depth, finish, 0)

    def finish_z(u, carry):
        z_copy(u).wait_send()
        return carry

    lax.fori_loop(0, depth - 1, finish_z, 0)


def fused_outputs(activations, gradients, act_history, grad_history, owner_rank, history_slot):
    dp, tensor = lax.axis_size("dp"), lax.axis_size("tensor")
    tokens, width = activations.shape
    rows, cols = gradients.shape
    hist = act_history.shape[1]
    depth = dp // (CORES * ROWS_Y)
    steps = depth * ROWS_Y
    block = width // dp
    loads = max(n for n in range(1, 13) if (cols // SUBLANES) % n == 0)
    padded = pl.cdiv(cols, LANES) * LANES
    dma = pltpu.SemaphoreType.DMA
    vmem = pl.BlockSpec(memory_space=pltpu.VMEM)
    hbm = pl.BlockSpec(memory_space=pl.ANY)
    f32, bf16 = jnp.float32, jnp.bfloat16
    others = tensor - 1
    return pl.pallas_call(
        functools.partial(fused_kernel, dp, tensor),
        out_shape=(
            jax.ShapeDtypeStruct((block, cols), f32),
            jax.ShapeDtypeStruct((1, hist, width), f32),
            jax.ShapeDtypeStruct((hist, cols), f32),
        ),
        in_specs=[hbm, hbm, vmem, vmem, vmem, vmem],
        out_specs=(vmem, vmem, vmem),
        scratch_shapes=[
            pltpu.VMEM((tokens, width), bf16),
            pltpu.VMEM((others, tokens, width), bf16),
            pltpu.VMEM((others, hist, width), f32),
            pltpu.VMEM((cols, rows), bf16),
            pltpu.VMEM((depth, ROWS_Y * CORES * block, cols), f32),
            pltpu.VMEM((steps, block, cols), f32),
            pltpu.VMEM((depth, block, cols), bf16),
            pltpu.VMEM((depth, block, cols), bf16),
            pltpu.VMEM((depth, block, cols), bf16),
            pltpu.VMEM((depth, block, cols), bf16),
            pltpu.VMEM((ROWS_Y * CORES * block, tokens), bf16),
            pltpu.VMEM((dp, 1, width + padded), f32),
            pltpu.VMEM((tensor, 1, width), f32),
            pltpu.VMEM((1, width), f32),
            pltpu.VMEM((1, padded), f32),
            pltpu.VMEM((padded, LANES), f32),
            pltpu.VMEM((padded, LANES), f32),
            pltpu.VMEM((block, LANES), f32),
            pltpu.VMEM((hist, width), f32),
            dma, dma((loads,)), dma((others,)), dma((others,)),
            dma((others, steps)), dma((others, steps)), dma((steps,)), dma((steps,)),
            dma((depth,)), dma((depth,)), dma((depth,)), dma((depth,)),
            dma((dp - 1,)), dma((dp - 1,)), dma((others,)), dma((others,)),
        ],
        compiler_params=pltpu.CompilerParams(
            collective_id=0, has_side_effects=True, vmem_limit_bytes=60 * 1024 * 1024
        ),
    )(
        activations, gradients.T, act_history, grad_history,
        owner_rank[None, :], history_slot[None, :],
    )


def hand_over_kernel(*refs):
    half = len(refs) // 2
    for source, target in zip(refs[:half], refs[half:]):
        target[...] = source[...]


def hand_over(*results):
    vmem = pl.BlockSpec(memory_space=pltpu.VMEM)
    return pl.pallas_call(
        hand_over_kernel,
        out_shape=tuple(jax.ShapeDtypeStruct(r.shape, r.dtype) for r in results),
        in_specs=[vmem] * len(results),
        out_specs=(vmem,) * len(results),
        compiler_params=pltpu.CompilerParams(vmem_limit_bytes=4 * 1024 * 1024),
    )(*results)


def gathered_sums(activations, gradients, act_history, grad_history, owner_rank):
    my_rank = lax.axis_index("tensor")
    held = jnp.where(owner_rank[None, :] == my_rank, act_history[0], jnp.float32(0.0))
    current = lax.psum(held, "tensor")
    act_scale = QUANT_LIMIT / jnp.maximum(jnp.max(current, axis=0), SCALE_FLOOR)
    grad_scale = QUANT_LIMIT / jnp.maximum(jnp.max(grad_history, axis=0), SCALE_FLOOR)
    gathered_rows = lax.all_gather(quantize(activations, act_scale), "tensor", axis=0, tiled=True)
    summed = lax.psum_scatter(
        lax.dot_general(
            gathered_rows, quantize(gradients, grad_scale), (((0,), (0,)), ((), ())),
            preferred_element_type=jnp.float32,
        ),
        "dp", scatter_dimension=0, tiled=True,
    )
    act_peak = lax.pmax(jnp.max(jnp.abs(activations), axis=0).astype(jnp.float32), ("dp", "tensor"))
    grad_peak = lax.pmax(jnp.max(jnp.abs(gradients), axis=0).astype(jnp.float32), "dp")
    return summed, current, act_peak[None, :], grad_peak[None, :]


def body(activations, gradients, act_history, grad_history, owner_rank, history_slot):
    dp = lax.axis_size("dp")
    model_width = act_history.shape[2]
    column_total = gradients.shape[1]
    row_count = model_width // dp
    fits = dp % (CORES * ROWS_Y) == 0 and (row_count * CORES) % LANES == 0
    fits = fits and column_total % SUBLANES == 0
    if fits:
        return hand_over(*fused_outputs(
            activations, gradients, act_history, grad_history, owner_rank, history_slot
        ))
    act_slots = history_slot[:model_width]
    grad_slots = lax.dynamic_slice_in_dim(
        history_slot, model_width + lax.axis_index("tensor") * column_total, column_total, 0
    )
    summed, current, act_peak, grad_peak = gathered_sums(
        activations, gradients, act_history, grad_history, owner_rank
    )
    act_scale = QUANT_LIMIT / jnp.maximum(jnp.max(current, axis=0), SCALE_FLOOR)
    grad_scale = QUANT_LIMIT / jnp.maximum(jnp.max(grad_history, axis=0), SCALE_FLOOR)
    grad_factor = 1.0 / math.sqrt(gradients.shape[0] * dp)
    row_base = lax.axis_index("dp") * row_count
    row_scale = lax.dynamic_slice_in_dim(act_scale, row_base, row_count, 0)
    weight_grad = summed / (row_scale[:, None] * grad_scale[None, :]) * grad_factor
    act_history_out = place_peaks(current, act_peak[0], act_slots)[None]
    grad_history_out = place_peaks(grad_history, grad_peak[0], grad_slots)
    return (weight_grad, act_history_out, grad_history_out)


def solution(mesh):
    placed = (
        P(("dp", "tensor"), None),
        P("dp", "tensor"),
        P("tensor", None, None),
        P(None, "tensor"),
        P(),
        P(),
    )
    return jax.shard_map(
        body,
        mesh=mesh,
        in_specs=placed,
        out_specs=(P("dp", "tensor"), P("tensor", None, None), P(None, "tensor")),
        check_vma=False,
    )
```
